32 devices in a mesh: dp: 4 (over x, core), vocab: 8 (over z, y).
Axes of the slice: x: 2, y: 2, z: 4, core: 2. Of those that a mesh axis runs over, the one named last changes fastest.
Arguments:
- hidden: bfloat16 [1024, 2048], P('dp', 'vocab'), may hold values from -30 to 30
- table: bfloat16 [16000, 2048], P('vocab'), may hold values from -20 to 20
- targets: int32 [1024], P('dp'), may hold values from 0 to 15999
- input_ids: int32 [2048], P(('dp', 'vocab')), may hold values from 0 to 15999, as said below
- cotangent: bfloat16 [2048, 2048], P(('dp', 'vocab')), may hold values from -0.4375 to 0.4375
Outputs:
- token_loss: float32 [1024], P('dp')
- hidden_grad: bfloat16 [1024, 2048], P('dp', 'vocab')
- table_grad: bfloat16 [16000, 2048], P('vocab', 'dp')
The draws below stay inside these ranges and needn't reach their ends.
Inputs may be any that keep to these rules, and one draw needn't show every extreme that they name: `input_ids`: within the 64 rows of one device, at most 16 ids fall in any one block of 2000 consecutive ids (the rows of one index of vocab); in every draw some block receives exactly 16 ids from every device.
All inputs are finite; a program needn't handle non-finite values.
Results may differ from the reference program's by a relative error of at most 0.0034.
Values may be sent and summed in bfloat16 or wider, within the bound.
A program may use at most 128 MiB of HBM per device.

```python
import math
import jax
import jax.numpy as jnp
import numpy as np
from jax import lax

D = 2048
V_DEV = 2000
IN_DEV = 64
VOCAB = 16000
TOKENS = 1024
IN_TOK = 2048
CAP = 16
N_DP = 4
N_VOCAB = 8


def table_line(base_key, row_index):
    return jax.random.normal(jax.random.fold_in(base_key, row_index), (D,), jnp.float32)


def common_axis(key):
    raw = jax.random.normal(jax.random.fold_in(key, 601), (D,), jnp.float32)
    return raw / jnp.sqrt(jnp.sum(raw * raw))


def draw_table(key, part):
    base_key = jax.random.fold_in(key, 501)
    values = jax.vmap(lambda row_index: table_line(base_key, row_index))(jnp.arange(VOCAB))
    values = jnp.clip(values, -6.0, 6.0)
    favored_count = min(16, V_DEV // 2)
    picks = jax.random.randint(jax.random.fold_in(key, 602), (VOCAB, 1), 0, V_DEV) < favored_count
    levels = jax.random.uniform(jax.random.fold_in(key, 603), (VOCAB, 1), jnp.float32, 4.0, 7.0)
    direction = common_axis(key)
    values = jnp.where(picks, 0.5 * values + levels * direction[None, :], values)
    return values.astype(jnp.bfloat16)


def draw_hidden(key, part):
    spread = 0.9 * D ** (-0.5)
    direction = common_axis(key)
    noise = jnp.clip(jax.random.normal(jax.random.fold_in(key, 11), (TOKENS, D), jnp.float32), -6.0, 6.0)
    amounts = jnp.exp(jax.random.uniform(jax.random.fold_in(key, 14), (TOKENS, 1), jnp.float32, math.log(0.7), math.log(1.4)))
    values = noise * spread + amounts * direction[None, :]
    return values.astype(jnp.bfloat16)


def draw_input_ids(key, part):
    common = jax.random.fold_in(key, 777)
    forced = jax.random.randint(jax.random.fold_in(common, 1), (), 0, N_VOCAB)
    popular = jax.random.randint(jax.random.fold_in(common, 2), (N_VOCAB,), 0, 4) * 4096
    slot_total = N_VOCAB * CAP
    slot_owner = jnp.arange(slot_total) // CAP

    def one_block(block_index):
        block_key = jax.random.fold_in(common, block_index + 10)
        noise = jax.random.randint(jax.random.fold_in(block_key, 1), (slot_total,), 0, 4096)
        score = noise + popular[slot_owner] + jnp.where(slot_owner == forced, 65536, 0)
        distinct = score * slot_total + jnp.arange(slot_total)
        order = jnp.argsort(-distinct, stable=True)
        chosen = slot_owner[order[:IN_DEV]]
        chosen = jax.random.permutation(jax.random.fold_in(block_key, 2), chosen)
        first_draw = jax.random.randint(jax.random.fold_in(block_key, 3), (IN_DEV,), 0, V_DEV)
        second_draw = jax.random.randint(jax.random.fold_in(block_key, 4), (IN_DEV,), 0, V_DEV)
        offset = first_draw * second_draw // V_DEV
        return chosen * V_DEV + offset
    blocks = jax.vmap(one_block)(jnp.arange(N_DP * N_VOCAB))
    return blocks.reshape(-1).astype(jnp.int32)


def place_ends(values, stream_key, low, largest):
    longest = values.shape.index(max(values.shape))
    spots = []
    for shift in (0, 1):
        where = [jax.random.randint(jax.random.fold_in(stream_key, axis), (), 0, length) for axis, length in enumerate(values.shape)]
        where[longest] = (where[longest] + shift) % values.shape[longest]
        spots.append(tuple(where))
    return values.at[spots[0]].set(low).at[spots[1]].set(largest)


def steps_of(rng, shape, shards, low, top_value):
    level = 1.0
    for axis_at, parts in shards:
        steps = jax.random.uniform(jax.random.fold_in(jax.random.fold_in(rng, 6), axis_at), (parts,), jnp.float32, low / len(shards), top_value / len(shards))
        level = level * jnp.repeat(jnp.exp(steps), shape[axis_at] // parts).reshape((-1,) + (1,) * (len(shape) - 1 - axis_at))
    return level


def cumulative_ranks(amount, slope):
    portions = [(1 << 20) // math.isqrt(grade ** slope) + 1 for grade in range(1, amount + 1)]
    scale = 1 + sum(portions) // (1 << 30)
    return np.cumsum(np.array([max(1, weight // scale) for weight in portions]))


def ranked_ids(own_key, shape, amount, skew):
    grid = cumulative_ranks(amount, skew)
    ticket = jax.random.randint(jax.random.fold_in(own_key, 1), shape, 0, int(grid[amount - 1]))
    rank = jnp.searchsorted(jnp.asarray(grid, jnp.int32), ticket, side="right")
    return jax.random.permutation(jax.random.fold_in(own_key, 2), amount)[rank].astype(jnp.int32)


def centred(own_key, dims, scale, bound, cuts=(), kind=jnp.bfloat16):
    loudness = steps_of(own_key, dims, cuts, -0.22, 0.18) if cuts else 1.0
    values = jax.random.normal(own_key, dims, jnp.float32) * scale * loudness
    return jnp.minimum(jnp.maximum(values, -bound), bound).astype(kind)


def setup_inputs(seed: int = 0) -> dict:
    arg_keys = jax.random.split(jax.random.key(seed), 6)
    return {
        "hidden": draw_hidden(jax.random.fold_in(arg_keys[5], 71), 0),
        "table": draw_table(jax.random.fold_in(arg_keys[5], 71), 0),
        "targets": place_ends(ranked_ids(arg_keys[2], (TOKENS,), VOCAB, 1), jax.random.fold_in(arg_keys[2], 3), 0, VOCAB - 1).astype(jnp.int32),
        "input_ids": draw_input_ids(jax.random.fold_in(arg_keys[5], 71), 0),
        "cotangent": centred(arg_keys[4], (IN_TOK, D), 0.03, 0.4375, ((0, 32),)),
    }


def reference(hidden, table, targets, input_ids, cotangent):
    blocks = table.reshape(N_VOCAB, V_DEV, D)
    starts = jnp.arange(N_VOCAB, dtype=jnp.int32) * V_DEV
    cot_wide = cotangent.astype(jnp.float32)

    def block_logits(rows):
        return lax.dot_general(hidden, rows, (((1,), (1,)), ((), ())), preferred_element_type=jnp.float32)

    def stats_step(carry, item):
        running_max, running_sum, target_logit = carry
        rows, first_row = item
        logits = block_logits(rows)
        columns = lax.broadcasted_iota(jnp.int32, logits.shape, 1) + first_row
        target_logit = target_logit + jnp.sum(jnp.where(columns == targets[:, None], logits, 0.0), axis=1)
        new_max = jnp.maximum(running_max, jnp.max(logits, axis=1))
        running_sum = running_sum * jnp.exp(running_max - new_max) + jnp.sum(jnp.exp(logits - new_max[:, None]), axis=1)
        return (new_max, running_sum, target_logit), None

    start_carry = (jnp.full((TOKENS,), -jnp.inf, jnp.float32), jnp.zeros((TOKENS,), jnp.float32), jnp.zeros((TOKENS,), jnp.float32))
    (row_max, row_sum, target_logit), unused = lax.scan(stats_step, start_carry, (blocks, starts))
    token_loss = row_max + jnp.log(row_sum) - target_logit

    def grad_step(hidden_acc, item):
        rows, first_row = item
        logits = block_logits(rows)
        columns = lax.broadcasted_iota(jnp.int32, logits.shape, 1) + first_row
        residual = (jnp.exp(logits - row_max[:, None]) / row_sum[:, None] - jnp.where(columns == targets[:, None], 1.0, 0.0)).astype(jnp.bfloat16)
        hidden_acc = hidden_acc + jnp.dot(residual, rows, preferred_element_type=jnp.float32)
        local_ids = input_ids - first_row
        local_ids = jnp.where((local_ids >= 0) & (local_ids < V_DEV), local_ids, V_DEV).astype(jnp.int32)
        scattered = jax.ops.segment_sum(cot_wide, local_ids, num_segments=V_DEV + 1)[:V_DEV]
        table_part = lax.dot_general(residual, hidden, (((0,), (0,)), ((), ())), preferred_element_type=jnp.float32) + scattered
        return hidden_acc, table_part.astype(jnp.bfloat16)

    hidden_acc, table_parts = lax.scan(grad_step, jnp.zeros((TOKENS, D), jnp.float32), (blocks, starts))
    return token_loss, hidden_acc.astype(jnp.bfloat16), table_parts.reshape(VOCAB, D)
```

```python
import functools

import jax
import jax.numpy as jnp
from jax import lax
from jax.experimental import pallas as pl
from jax.experimental.pallas import tpu as pltpu
from jax.sharding import PartitionSpec as P

MESH = pl.DeviceIdType.MESH
VMEM_LIMIT = 58 * 1024 * 1024


def remote(src, dst, send_sem, recv_sem, device):
    return pltpu.make_async_remote_copy(
        src_ref=src,
        dst_ref=dst,
        send_sem=send_sem,
        recv_sem=recv_sem,
        device_id=device,
        device_id_type=MESH,
    )


def greet(devices):
    barrier = pltpu.get_barrier_semaphore()
    for device in devices:
        pl.semaphore_signal(barrier, inc=1, device_id=device, device_id_type=MESH)
    pl.semaphore_wait(barrier, len(devices))


def gather_kernel(
    n_d, n_v, own_ref, full_ref, block_ref, local_sem, own_sem,
    send_sem, recv_sem, pass_sem, got_sem, block_send, block_recv,
):
    d = lax.axis_index("dp")
    v = lax.axis_index("vocab")
    half = n_v // 2
    per = n_v // n_d
    partner = v + 1 - 2 * lax.rem(v, 2)

    def same(step):
        return lax.rem(v + 2 * step, n_v)

    def across(step):
        return lax.rem(partner + 2 * step, n_v)

    devices = [(d, same(s)) for s in range(1, half)] + [(d, partner)]
    devices += [(lax.rem(d + t, n_d), v) for t in range(1, n_d)]
    greet(devices)

    started = []
    directs = []
    for s in range(1, half):
        copy = remote(own_ref, full_ref.at[v], send_sem.at[s], recv_sem.at[s], (d, same(s)))
        copy.start()
        directs.append(copy)
    local = pltpu.make_async_copy(own_ref, full_ref.at[v], local_sem)
    local.start()

    def relay(step, index, source):
        copy = remote(source, full_ref.at[index], pass_sem.at[step], got_sem.at[step], (d, partner))
        copy.start()
        started.append(copy)

    sends = []

    def to_block(slot, index, source):
        owner = index // per
        place = index - owner * per
        shift = lax.rem(owner - d + n_d, n_d)
        away = owner != d
        out = remote(
            source,
            block_ref.at[d, place],
            block_send.at[slot],
            block_recv.at[shift, place],
            (owner, v),
        )
        keep = pltpu.make_async_copy(source, block_ref.at[d, place], own_sem.at[slot])

        @pl.when(away)
        def _():
            out.start()

        @pl.when(jnp.logical_not(away))
        def _():
            keep.start()

        sends.append((away, out, keep))

    relay(0, v, own_ref)
    to_block(0, v, own_ref)
    for s in range(1, half):
        index = lax.rem(v - 2 * s + 2 * n_v, n_v)
        directs[s - 1].wait_recv()
        relay(s, index, full_ref.at[index])
        to_block(s, index, full_ref.at[index])
    for s in range(half):
        index = lax.rem(partner - 2 * s + 2 * n_v, n_v)
        started[s].wait_recv()
        to_block(half + s, index, full_ref.at[index])
    local.wait()
    for away, out, keep in sends:

        @pl.when(away)
        def _():
            out.wait_send()

        @pl.when(jnp.logical_not(away))
        def _():
            keep.wait()

    for copy in directs + started:
        copy.wait_send()
    for t in range(1, n_d):
        source = lax.rem(d - t + n_d, n_d)
        for place in range(per):
            remote(
                own_ref, block_ref.at[source, place], block_send.at[0],
                block_recv.at[t, place], (source, v),
            ).wait_recv()


def gather(hidden, n_d, n_v):
    rows, width = hidden.shape
    half = n_v // 2
    per = n_v // n_d
    vmem = pl.BlockSpec(memory_space=pltpu.VMEM)
    return pl.pallas_call(
        functools.partial(gather_kernel, n_d, n_v),
        out_shape=(
            jax.ShapeDtypeStruct((n_v, rows, width), hidden.dtype),
            jax.ShapeDtypeStruct((n_d, per, rows, width), hidden.dtype),
        ),
        in_specs=[vmem],
        out_specs=(vmem, vmem),
        scratch_shapes=[
            pltpu.SemaphoreType.DMA,
            pltpu.SemaphoreType.DMA((n_v,)),
            pltpu.SemaphoreType.DMA((half,)),
            pltpu.SemaphoreType.DMA((half,)),
            pltpu.SemaphoreType.DMA((half,)),
            pltpu.SemaphoreType.DMA((half,)),
            pltpu.SemaphoreType.DMA((n_v,)),
            pltpu.SemaphoreType.DMA((n_d, per)),
        ],
        compiler_params=pltpu.CompilerParams(
            collective_id=0, has_side_effects=True, vmem_limit_bytes=VMEM_LIMIT
        ),
    )(hidden)


def stats_kernel(n_v, own_ref, all_ref, local_sem, send_sem, recv_sem):
    d = lax.axis_index("dp")
    v = lax.axis_index("vocab")
    greet([(d, lax.rem(v + s, n_v)) for s in range(1, n_v)])
    copies = []
    for s in range(1, n_v):
        copy = remote(
            own_ref, all_ref.at[v], send_sem.at[s], recv_sem.at[s], (d, lax.rem(v + s, n_v))
        )
        copy.start()
        copies.append(copy)
    local = pltpu.make_async_copy(own_ref, all_ref.at[v], local_sem)
    local.start()
    local.wait()
    for copy in copies:
        copy.wait()


def exchange_stats(stats, n_v):
    vmem = pl.BlockSpec(memory_space=pltpu.VMEM)
    return pl.pallas_call(
        functools.partial(stats_kernel, n_v),
        out_shape=jax.ShapeDtypeStruct((n_v,) + stats.shape, stats.dtype),
        in_specs=[vmem],
        out_specs=vmem,
        scratch_shapes=[
            pltpu.SemaphoreType.DMA,
            pltpu.SemaphoreType.DMA((n_v,)),
            pltpu.SemaphoreType.DMA((n_v,)),
        ],
        compiler_params=pltpu.CompilerParams(collective_id=1, has_side_effects=True),
    )(stats)


def final_kernel(
    n_d, n_v, reduces, res_ref, table_ref, rows_ref, ids_ref,
    grad_ref, all_ref, got_rows_ref, got_ids_ref,
    pair_out, pair_in, sums, cross_out, cross_in,
    local_sem, res_send, res_recv, pass_send, pass_recv,
    pair_send, pair_recv, cross_send, cross_recv,
    row_send, row_recv, id_send, id_recv,
):
    d = lax.axis_index("dp")
    v = lax.axis_index("vocab")
    half = n_v // 2
    half_d = n_d // 2
    mate = d + 1 - 2 * lax.rem(d, 2)
    partner = v + 1 - 2 * lax.rem(v, 2)
    total = n_d * n_v
    me = d * n_v + v

    def place(step):
        other = lax.rem(me + step, total)
        return other // n_v, lax.rem(other, n_v)

    greet([place(s) for s in range(1, total)])

    directs = []
    for s in range(1, half_d):
        copy = remote(
            res_ref, all_ref.at[d], res_send.at[s], res_recv.at[s], (lax.rem(d + 2 * s, n_d), v)
        )
        copy.start()
        directs.append(copy)
    passes = [remote(res_ref, all_ref.at[d], pass_send.at[0], pass_recv.at[0], (mate, v))]
    passes[0].start()
    locals_ = [
        pltpu.make_async_copy(res_ref, all_ref.at[d], local_sem.at[0]),
        pltpu.make_async_copy(rows_ref.at[d, v], got_rows_ref.at[d, v], local_sem.at[1]),
        pltpu.make_async_copy(ids_ref.at[v], got_ids_ref.at[d, v], local_sem.at[2]),
    ]
    for copy in locals_:
        copy.start()

    order = [(s + 1) % half for s in range(half)]
    width = table_ref.shape[1] // n_v

    def product(index):
        return jnp.dot(
            res_ref[...],
            table_ref[:, pl.ds(pl.multiple_of(index * width, 128), width)],
            preferred_element_type=jnp.float32,
        )

    pairs = {}
    if reduces:
        for s in order:
            pair_out[s] = product(lax.rem(partner + 2 * s, n_v))
            pairs[s] = remote(
                pair_out.at[s], pair_in.at[s], pair_send.at[s], pair_recv.at[s], (d, partner)
            )
            pairs[s].start()

    shuffles = []
    for s in range(1, total):
        to_d, to_v = place(s)
        for copy in (
            remote(
                rows_ref.at[to_d, to_v], got_rows_ref.at[d, v], row_send.at[s], row_recv.at[s],
                (to_d, to_v),
            ),
            remote(
                ids_ref.at[to_v], got_ids_ref.at[d, v], id_send.at[s], id_recv.at[s], (to_d, to_v)
            ),
        ):
            copy.start()
            shuffles.append(copy)

    crosses = []
    if reduces:
        for s in order:
            sums[s] = product(lax.rem(v + 2 * s, n_v))
        for s in order:
            pairs[s].wait_recv()
            if s == 0:
                continue
            cross_out[s] = (sums[s] + pair_in[s]).astype(jnp.bfloat16)
            copy = remote(
                cross_out.at[s], cross_in.at[s], cross_send.at[s], cross_recv.at[s],
                (d, lax.rem(v + 2 * s, n_v)),
            )
            copy.start()
            crosses.append(copy)

    for s in range(1, half_d):
        source = lax.rem(d - 2 * s + 2 * n_d, n_d)
        directs[s - 1].wait_recv()
        copy = remote(
            all_ref.at[source], all_ref.at[source], pass_send.at[s], pass_recv.at[s], (mate, v)
        )
        copy.start()
        passes.append(copy)

    if reduces:
        value = sums[0] + pair_in[0]
        for s, copy in zip(order, crosses):
            copy.wait_recv()
            value = value + cross_in[s].astype(jnp.float32)
        grad_ref[...] = value.astype(jnp.bfloat16)
    else:
        grad_ref[...] = jnp.zeros_like(grad_ref)

    for copy in locals_:
        copy.wait()
    for copy in passes:
        copy.wait()
    for copy in directs + crosses + list(pairs.values()):
        copy.wait_send()
    for copy in shuffles:
        copy.wait()


def finish(residual, table, send_rows, send_ids, n_d, n_v):
    rows = residual.shape[0]
    width = table.shape[1] // n_v
    reduces = width % 128 == 0
    half = n_v // 2
    total = n_d * n_v
    kept = width if reduces else 128
    slots = half if reduces else 1
    if not reduces:
        table = table[:8, :n_v * 128]
    vmem = pl.BlockSpec(memory_space=pltpu.VMEM)
    dma = pltpu.SemaphoreType.DMA
    results = pl.pallas_call(
        functools.partial(final_kernel, n_d, n_v, reduces),
        out_shape=(
            jax.ShapeDtypeStruct((rows, kept), jnp.bfloat16),
            jax.ShapeDtypeStruct((n_d,) + residual.shape, residual.dtype),
            jax.ShapeDtypeStruct(send_rows.shape, send_rows.dtype),
            jax.ShapeDtypeStruct((n_d,) + send_ids.shape, send_ids.dtype),
        ),
        in_specs=[vmem] * 4,
        out_specs=(vmem,) * 4,
        scratch_shapes=[
            pltpu.VMEM((slots, rows, kept), jnp.float32),
            pltpu.VMEM((slots, rows, kept), jnp.float32),
            pltpu.VMEM((slots, rows, kept), jnp.float32),
            pltpu.VMEM((slots, rows, kept), jnp.bfloat16),
            pltpu.VMEM((slots, rows, kept), jnp.bfloat16),
            dma((3,)),
            dma((n_d,)), dma((n_d,)), dma((n_d,)), dma((n_d,)),
            dma((half,)), dma((half,)), dma((half,)), dma((half,)),
            dma((total,)), dma((total,)), dma((total,)), dma((total,)),
        ],
        compiler_params=pltpu.CompilerParams(
            collective_id=2, has_side_effects=True, vmem_limit_bytes=VMEM_LIMIT
        ),
    )(residual, table, send_rows, send_ids)
    return reduces, results


def body(hidden, table, targets, input_ids, cotangent):
    vocab_rows, model_width = table.shape
    n_d = lax.axis_size("dp")
    n_v = lax.axis_size("vocab")
    tokens = hidden.shape[0]
    first_row = lax.axis_index("vocab") * vocab_rows
    block_width = model_width // n_d

    pieces, blocks = gather(hidden, n_d, n_v)
    hidden_full = jnp.transpose(pieces, (1, 0, 2)).reshape(tokens, model_width)
    hidden_block = jnp.transpose(blocks, (0, 2, 1, 3)).reshape(n_d * tokens, block_width)

    logits = lax.dot_general(
        hidden_full, table, (((1,), (1,)), ((), ())), preferred_element_type=jnp.float32
    )
    columns = lax.broadcasted_iota(jnp.int32, logits.shape, 1)
    is_target = columns == (targets - first_row)[:, None]
    picked = jnp.sum(jnp.where(is_target, logits, 0.0), axis=1)
    local_max = jnp.max(logits, axis=1)
    shifted = jnp.exp(logits - local_max[:, None])
    local_sum = jnp.sum(shifted, axis=1)
    stats = jnp.stack([local_max, local_sum, picked] + [picked] * 5)
    shared = exchange_stats(stats, n_v)
    maxima, sums = shared[:, 0], shared[:, 1]
    row_max = jnp.max(maxima, axis=0)
    row_sum = jnp.sum(sums * jnp.exp(maxima - row_max[None, :]), axis=0)
    target_logit = jnp.sum(shared[:, 2], axis=0)
    token_loss = row_max + jnp.log(row_sum) - target_logit
    residual = (
        jnp.exp(logits - row_max[:, None]) / row_sum[:, None] - jnp.where(is_target, 1.0, 0.0)
    ).astype(jnp.bfloat16)

    row_count = input_ids.shape[0]
    capacity = max(2, 2 * row_count // n_v)
    slot_total = n_v * capacity
    owners = input_ids // vocab_rows
    offsets = input_ids - owners * vocab_rows
    later_rows = lax.broadcasted_iota(jnp.int32, (row_count, row_count), 0)
    earlier_rows = lax.broadcasted_iota(jnp.int32, (row_count, row_count), 1)
    earlier = (owners[:, None] == owners[None, :]) & (earlier_rows < later_rows)
    position = jnp.sum(earlier.astype(jnp.int32), axis=1)
    slot_index = owners * capacity + position
    selector = lax.broadcasted_iota(jnp.int32, (slot_total, row_count), 0) == slot_index[None, :]
    packed = jnp.dot(
        selector.astype(jnp.bfloat16), cotangent, preferred_element_type=jnp.float32
    ).astype(jnp.bfloat16)
    send_rows = jnp.transpose(packed.reshape(n_v, capacity, n_d, block_width), (2, 0, 1, 3))
    send_offsets = jnp.sum(jnp.where(selector, offsets[None, :] + 1, 0), axis=1) - 1
    send_ids = jnp.pad(
        send_offsets.reshape(n_v, 1, capacity), ((0, 0), (0, 0), (0, 128 - capacity)),
        constant_values=-1,
    )

    reduces, (grad, res_all, got_rows, got_ids) = finish(
        residual, table, send_rows, send_ids, n_d, n_v
    )
    if reduces:
        hidden_grad = grad
    else:
        hidden_part = jnp.dot(residual, table, preferred_element_type=jnp.float32)
        hidden_grad = lax.psum_scatter(
            hidden_part, "vocab", scatter_dimension=1, tiled=True
        ).astype(jnp.bfloat16)

    flat_rows = got_rows.reshape(-1, block_width)
    flat_offsets = got_ids[:, :, 0, :capacity].reshape(-1)
    matches = (
        lax.broadcasted_iota(jnp.int32, (vocab_rows, flat_offsets.shape[0]), 0)
        == flat_offsets[None, :]
    )
    start_sum = jnp.dot(matches.astype(jnp.bfloat16), flat_rows, preferred_element_type=jnp.float32)
    table_sum = start_sum + lax.dot_general(
        res_all.reshape(n_d * tokens, vocab_rows),
        hidden_block,
        (((0,), (0,)), ((), ())),
        preferred_element_type=jnp.float32,
    )
    return (token_loss, hidden_grad, table_sum.astype(jnp.bfloat16))


def solution(mesh):
    placed = (
        P("dp", "vocab"),
        P("vocab", None),
        P("dp"),
        P(("dp", "vocab")),
        P(("dp", "vocab"), None),
    )
    return jax.shard_map(
        body,
        mesh=mesh,
        in_specs=placed,
        out_specs=(P("dp"), P("dp", "vocab"), P("vocab", "dp")),
        check_vma=False,
    )
```

```python
import functools

import jax
import jax.numpy as jnp
from jax import lax
from jax.experimental import pallas as pl
from jax.experimental.pallas import tpu as pltpu
from jax.sharding import PartitionSpec as P

MESH = pl.DeviceIdType.MESH
VMEM_LIMIT = 58 * 1024 * 1024


def remote(src, dst, send_sem, recv_sem, device):
    return pltpu.make_async_remote_copy(
        src_ref=src,
        dst_ref=dst,
        send_sem=send_sem,
        recv_sem=recv_sem,
        device_id=device,
        device_id_type=MESH,
    )


def greet(devices):
    barrier = pltpu.get_barrier_semaphore()
    for device in devices:
        pl.semaphore_signal(barrier, inc=1, device_id=device, device_id_type=MESH)
    pl.semaphore_wait(barrier, len(devices))


def gather_kernel(
    n_d, n_v, own_ref, full_ref, block_ref, local_sem, own_sem,
    send_sem, recv_sem, pass_sem, got_sem, block_send, block_recv,
):
    d = lax.axis_index("dp")
    v = lax.axis_index("vocab")
    half = n_v // 2
    per = n_v // n_d
    partner = v + 1 - 2 * lax.rem(v, 2)

    width = own_ref.shape[1]
    aligned = width % 128 == 0

    def piece(index):
        if aligned:
            return full_ref.at[:, pl.ds(pl.multiple_of(index * width, 128), width)]
        return full_ref.at[index]

    def part(group, spot):
        if aligned:
            return block_ref.at[group, :, pl.ds(pl.multiple_of(spot * width, 128), width)]
        return block_ref.at[group, spot]

    def same(step):
        return lax.rem(v + 2 * step, n_v)

    devices = [(d, same(s)) for s in range(1, half)] + [(d, partner)]
    devices += [(lax.rem(d + t, n_d), v) for t in range(1, n_d)]
    greet(devices)

    started = []
    directs = []
    for s in range(1, half):
        copy = remote(own_ref, piece(v), send_sem.at[s], recv_sem.at[s], (d, same(s)))
        copy.start()
        directs.append(copy)
    local = pltpu.make_async_copy(own_ref, piece(v), local_sem)
    local.start()

    def relay(step, index, source):
        copy = remote(source, piece(index), pass_sem.at[step], got_sem.at[step], (d, partner))
        copy.start()
        started.append(copy)

    sends = []

    def to_block(slot, index, source):
        owner = index // per
        place = index - owner * per
        shift = lax.rem(owner - d + n_d, n_d)
        away = owner != d
        out = remote(
            source,
            part(d, place),
            block_send.at[slot],
            block_recv.at[shift, place],
            (owner, v),
        )
        keep = pltpu.make_async_copy(source, part(d, place), own_sem.at[slot])

        @pl.when(away)
        def _():
            out.start()

        @pl.when(jnp.logical_not(away))
        def _():
            keep.start()

        sends.append((away, out, keep))

    relay(0, v, own_ref)
    to_block(0, v, own_ref)
    for s in range(1, half):
        index = lax.rem(v - 2 * s + 2 * n_v, n_v)
        directs[s - 1].wait_recv()
        relay(s, index, piece(index))
        to_block(s, index, piece(index))
    for s in range(half):
        index = lax.rem(partner - 2 * s + 2 * n_v, n_v)
        started[s].wait_recv()
        to_block(half + s, index, piece(index))
    local.wait()
    for away, out, keep in sends:

        @pl.when(away)
        def _():
            out.wait_send()

        @pl.when(jnp.logical_not(away))
        def _():
            keep.wait()

    for copy in directs + started:
        copy.wait_send()
    for t in range(1, n_d):
        source = lax.rem(d - t + n_d, n_d)
        for place in range(per):
            remote(
                own_ref, part(source, place), block_send.at[0],
                block_recv.at[t, place], (source, v),
            ).wait_recv()


def gather(hidden, n_d, n_v):
    rows, width = hidden.shape
    half = n_v // 2
    per = n_v // n_d
    full_shape = (n_v, rows, width)
    block_shape = (n_d, per, rows, width)
    if width % 128 == 0:
        full_shape = (rows, n_v * width)
        block_shape = (n_d, rows, per * width)
    vmem = pl.BlockSpec(memory_space=pltpu.VMEM)
    return pl.pallas_call(
        functools.partial(gather_kernel, n_d, n_v),
        out_shape=(
            jax.ShapeDtypeStruct(full_shape, hidden.dtype),
            jax.ShapeDtypeStruct(block_shape, hidden.dtype),
        ),
        in_specs=[vmem],
        out_specs=(vmem, vmem),
        scratch_shapes=[
            pltpu.SemaphoreType.DMA,
            pltpu.SemaphoreType.DMA((n_v,)),
            pltpu.SemaphoreType.DMA((half,)),
            pltpu.SemaphoreType.DMA((half,)),
            pltpu.SemaphoreType.DMA((half,)),
            pltpu.SemaphoreType.DMA((half,)),
            pltpu.SemaphoreType.DMA((n_v,)),
            pltpu.SemaphoreType.DMA((n_d, per)),
        ],
        compiler_params=pltpu.CompilerParams(
            collective_id=0, has_side_effects=True, vmem_limit_bytes=VMEM_LIMIT
        ),
    )(hidden)


def final_kernel(
    n_d, n_v, reduces, hid_ref, table_ref, target_ref, rows_ref, ids_ref,
    loss_ref, grad_ref, all_ref, got_rows_ref, got_ids_ref,
    logit_ref, res_ref, own_stats, all_stats, stat_local, stat_send, stat_recv,
    pair_out, pair_in, sums, cross_out, cross_in,
    local_sem, res_send, res_recv, pass_send, pass_recv,
    pair_send, pair_recv, cross_send, cross_recv,
    row_send, row_recv, id_send, id_recv,
):
    d = lax.axis_index("dp")
    v = lax.axis_index("vocab")
    half = n_v // 2
    half_d = n_d // 2
    mate = d + 1 - 2 * lax.rem(d, 2)
    partner = v + 1 - 2 * lax.rem(v, 2)
    total = n_d * n_v
    me = d * n_v + v

    def place(step):
        other = lax.rem(me + step, total)
        return other // n_v, lax.rem(other, n_v)

    greet([place(s) for s in range(1, total)])

    shuffles = []

    def shuffle(first):
        for s in range(first, total, 2):
            to_d, to_v = place(s)
            for copy in (
                remote(
                    rows_ref.at[to_d, to_v], got_rows_ref.at[d, v],
                    row_send.at[s], row_recv.at[s], (to_d, to_v),
                ),
                remote(
                    ids_ref.at[to_v], got_ids_ref.at[d, v],
                    id_send.at[s], id_recv.at[s], (to_d, to_v),
                ),
            ):
                copy.start()
                shuffles.append(copy)

    shuffle(1)
    tokens, vocab_rows = res_ref.shape
    target = target_ref[...]
    chunks = [(c, min(256, vocab_rows - c)) for c in range(0, vocab_rows, 256)]

    def hits(start, size):
        return lax.broadcasted_iota(jnp.int32, (tokens, size), 1) + start == target

    peak = jnp.full((tokens, 1), -jnp.inf, jnp.float32)
    picked = jnp.zeros((tokens, 1), jnp.float32)
    for start, size in chunks:
        value = lax.dot_general(
            hid_ref[...], table_ref[start:start + size, :], (((1,), (1,)), ((), ())),
            preferred_element_type=jnp.float32,
        )
        logit_ref[:, start:start + size] = value
        peak = jnp.maximum(peak, jnp.max(value, axis=1, keepdims=True))
        picked = picked + jnp.sum(
            jnp.where(hits(start, size), value, 0.0), axis=1, keepdims=True
        )
    amount = jnp.zeros((tokens, 1), jnp.float32)
    for start, size in chunks:
        value = jnp.exp(logit_ref[:, start:start + size] - peak)
        logit_ref[:, start:start + size] = value
        amount = amount + jnp.sum(value, axis=1, keepdims=True)
    lane = lax.broadcasted_iota(jnp.int32, (tokens, 128), 1)
    wide = jnp.where(lane == 0, peak, jnp.where(lane == 1, amount, picked))
    own_stats[...] = jnp.transpose(wide)[:8]
    stats = []
    for s in range(1, n_v):
        copy = remote(
            own_stats, all_stats.at[v], stat_send.at[s], stat_recv.at[s],
            (d, lax.rem(v + s, n_v)),
        )
        copy.start()
        stats.append(copy)
    keep_stats = pltpu.make_async_copy(own_stats, all_stats.at[v], stat_local)
    keep_stats.start()
    shuffle(2)
    keep_stats.wait()
    for copy in stats:
        copy.wait()
    row_max = all_stats[0, 0:1, :]
    for k in range(1, n_v):
        row_max = jnp.maximum(row_max, all_stats[k, 0:1, :])
    row_sum = jnp.zeros_like(row_max)
    target_logit = jnp.zeros_like(row_max)
    for k in range(n_v):
        row_sum = row_sum + all_stats[k, 1:2, :] * jnp.exp(all_stats[k, 0:1, :] - row_max)
        target_logit = target_logit + all_stats[k, 2:3, :]
    loss_ref[...] = row_max + jnp.log(row_sum) - target_logit
    factor = jnp.exp(own_stats[0:1, :] - row_max) / row_sum
    factor = jnp.transpose(jnp.broadcast_to(factor, (128, tokens)))[:, 0:1]
    for start, size in chunks:
        value = logit_ref[:, start:start + size] * factor
        value = value - jnp.where(hits(start, size), 1.0, 0.0)
        res_ref[:, start:start + size] = value.astype(jnp.bfloat16)

    directs = []
    for s in range(1, half_d):
        copy = remote(
            res_ref, all_ref.at[d], res_send.at[s], res_recv.at[s], (lax.rem(d + 2 * s, n_d), v)
        )
        copy.start()
        directs.append(copy)
    passes = [remote(res_ref, all_ref.at[d], pass_send.at[0], pass_recv.at[0], (mate, v))]
    passes[0].start()
    locals_ = [
        pltpu.make_async_copy(res_ref, all_ref.at[d], local_sem.at[0]),
        pltpu.make_async_copy(rows_ref.at[d, v], got_rows_ref.at[d, v], local_sem.at[1]),
        pltpu.make_async_copy(ids_ref.at[v], got_ids_ref.at[d, v], local_sem.at[2]),
    ]
    for copy in locals_:
        copy.start()

    order = [(s + 1) % half for s in range(half)]
    width = table_ref.shape[1] // n_v

    def product(index):
        return jnp.dot(
            res_ref[...],
            table_ref[:, pl.ds(pl.multiple_of(index * width, 128), width)],
            preferred_element_type=jnp.float32,
        )

    pairs = {}
    if reduces:
        for s in order:
            pair_out[s] = product(lax.rem(partner + 2 * s, n_v))
            pairs[s] = remote(
                pair_out.at[s], pair_in.at[s], pair_send.at[s], pair_recv.at[s], (d, partner)
            )
            pairs[s].start()

    crosses = []
    if reduces:
        for s in order:
            sums[s] = product(lax.rem(v + 2 * s, n_v))
        for s in order:
            pairs[s].wait_recv()
            if s == 0:
                continue
            cross_out[s] = (sums[s] + pair_in[s]).astype(jnp.bfloat16)
            copy = remote(
                cross_out.at[s], cross_in.at[s], cross_send.at[s], cross_recv.at[s],
                (d, lax.rem(v + 2 * s, n_v)),
            )
            copy.start()
            crosses.append(copy)

    for s in range(1, half_d):
        source = lax.rem(d - 2 * s + 2 * n_d, n_d)
        directs[s - 1].wait_recv()
        copy = remote(
            all_ref.at[source], all_ref.at[source], pass_send.at[s], pass_recv.at[s], (mate, v)
        )
        copy.start()
        passes.append(copy)

    if reduces:
        value = sums[0] + pair_in[0]
        for s, copy in zip(order, crosses):
            copy.wait_recv()
            value = value + cross_in[s].astype(jnp.float32)
        grad_ref[...] = value.astype(jnp.bfloat16)
    else:
        grad_ref[...] = jnp.zeros_like(grad_ref)

    for copy in locals_:
        copy.wait()
    for copy in passes:
        copy.wait()
    for copy in directs + crosses + list(pairs.values()):
        copy.wait_send()
    for copy in shuffles:
        copy.wait()


def finish(hidden_full, table, target, send_rows, send_ids, n_d, n_v):
    rows = hidden_full.shape[0]
    vocab_rows = table.shape[0]
    width = table.shape[1] // n_v
    reduces = width % 128 == 0
    half = n_v // 2
    total = n_d * n_v
    kept = width if reduces else 128
    slots = half if reduces else 1
    vmem = pl.BlockSpec(memory_space=pltpu.VMEM)
    dma = pltpu.SemaphoreType.DMA
    results = pl.pallas_call(
        functools.partial(final_kernel, n_d, n_v, reduces),
        out_shape=(
            jax.ShapeDtypeStruct((1, rows), jnp.float32),
            jax.ShapeDtypeStruct((rows, kept), jnp.bfloat16),
            jax.ShapeDtypeStruct((n_d, rows, vocab_rows), jnp.bfloat16),
            jax.ShapeDtypeStruct(send_rows.shape, send_rows.dtype),
            jax.ShapeDtypeStruct((n_d,) + send_ids.shape, send_ids.dtype),
        ),
        in_specs=[vmem] * 5,
        out_specs=(vmem,) * 5,
        scratch_shapes=[
            pltpu.VMEM((rows, vocab_rows), jnp.float32),
            pltpu.VMEM((rows, vocab_rows), jnp.bfloat16),
            pltpu.VMEM((8, rows), jnp.float32),
            pltpu.VMEM((n_v, 8, rows), jnp.float32),
            dma,
            dma((n_v,)),
            dma((n_v,)),
            pltpu.VMEM((slots, rows, kept), jnp.float32),
            pltpu.VMEM((slots, rows, kept), jnp.float32),
            pltpu.VMEM((slots, rows, kept), jnp.float32),
            pltpu.VMEM((slots, rows, kept), jnp.bfloat16),
            pltpu.VMEM((slots, rows, kept), jnp.bfloat16),
            dma((3,)),
            dma((n_d,)), dma((n_d,)), dma((n_d,)), dma((n_d,)),
            dma((half,)), dma((half,)), dma((half,)), dma((half,)),
            dma((total,)), dma((total,)), dma((total,)), dma((total,)),
        ],
        compiler_params=pltpu.CompilerParams(
            collective_id=1, has_side_effects=True, vmem_limit_bytes=VMEM_LIMIT
        ),
    )(hidden_full, table, target, send_rows, send_ids)
    return reduces, results


def body(hidden, table, targets, input_ids, cotangent):
    vocab_rows, model_width = table.shape
    n_d = lax.axis_size("dp")
    n_v = lax.axis_size("vocab")
    tokens = hidden.shape[0]
    first_row = lax.axis_index("vocab") * vocab_rows
    block_width = model_width // n_d

    pieces, blocks = gather(hidden, n_d, n_v)
    if hidden.shape[1] % 128 == 0:
        hidden_full = pieces
        hidden_block = blocks.reshape(n_d * tokens, block_width)
    else:
        hidden_full = jnp.transpose(pieces, (1, 0, 2)).reshape(tokens, model_width)
        hidden_block = jnp.transpose(blocks, (0, 2, 1, 3)).reshape(n_d * tokens, block_width)
    target = (targets - first_row)[:, None]

    row_count = input_ids.shape[0]
    capacity = max(2, 2 * row_count // n_v)
    slot_total = n_v * capacity
    owners = input_ids // vocab_rows
    offsets = input_ids - owners * vocab_rows
    later_rows = lax.broadcasted_iota(jnp.int32, (row_count, row_count), 0)
    earlier_rows = lax.broadcasted_iota(jnp.int32, (row_count, row_count), 1)
    earlier = (owners[:, None] == owners[None, :]) & (earlier_rows < later_rows)
    position = jnp.sum(earlier.astype(jnp.int32), axis=1)
    slot_index = owners * capacity + position
    selector = lax.broadcasted_iota(jnp.int32, (slot_total, row_count), 0) == slot_index[None, :]
    packed = jnp.dot(
        selector.astype(jnp.bfloat16), cotangent, preferred_element_type=jnp.float32
    ).astype(jnp.bfloat16)
    send_rows = jnp.transpose(packed.reshape(n_v, capacity, n_d, block_width), (2, 0, 1, 3))
    send_offsets = jnp.sum(jnp.where(selector, offsets[None, :] + 1, 0), axis=1) - 1
    send_ids = jnp.pad(
        send_offsets.reshape(n_v, 1, capacity), ((0, 0), (0, 0), (0, 128 - capacity)),
        constant_values=-1,
    )

    reduces, (loss, grad, res_all, got_rows, got_ids) = finish(
        hidden_full, table, target, send_rows, send_ids, n_d, n_v
    )
    if reduces:
        hidden_grad = grad
    else:
        residual = lax.dynamic_index_in_dim(res_all, lax.axis_index("dp"), 0, keepdims=False)
        hidden_part = jnp.dot(residual, table, preferred_element_type=jnp.float32)
        hidden_grad = lax.psum_scatter(
            hidden_part, "vocab", scatter_dimension=1, tiled=True
        ).astype(jnp.bfloat16)

    flat_rows = got_rows.reshape(-1, block_width)
    flat_offsets = got_ids[:, :, 0, :capacity].reshape(-1)
    matches = (
        lax.broadcasted_iota(jnp.int32, (vocab_rows, flat_offsets.shape[0]), 0)
        == flat_offsets[None, :]
    )
    start_sum = jnp.dot(matches.astype(jnp.bfloat16), flat_rows, preferred_element_type=jnp.float32)
    table_sum = start_sum + lax.dot_general(
        res_all.reshape(n_d * tokens, vocab_rows),
        hidden_block,
        (((0,), (0,)), ((), ())),
        preferred_element_type=jnp.float32,
    )
    return (loss[0], hidden_grad, table_sum.astype(jnp.bfloat16))


def solution(mesh):
    placed = (
        P("dp", "vocab"),
        P("vocab", None),
        P("dp"),
        P(("dp", "vocab")),
        P(("dp", "vocab"), None),
    )
    return jax.shard_map(
        body,
        mesh=mesh,
        in_specs=placed,
        out_specs=(P("dp"), P("dp", "vocab"), P("vocab", "dp")),
        check_vma=False,
    )
```
